32 devices in a mesh: dp: 4 (over z), row: 2 (over y), col: 4 (over x, core).
Axes of the slice: x: 2, y: 2, z: 4, core: 2. Of those that a mesh axis runs over, the one named last changes fastest.
Arguments:
- x_seq: bfloat16 [1024, 64, 576], P(('dp', 'row', 'col'))
- dy_seq: bfloat16 [1024, 64, 576], P(('dp', 'row', 'col'))
- w_query: bfloat16 [576, 9, 64], P(('row', 'col'))
- w_key: bfloat16 [576, 3, 64], P(('row', 'col'))
- w_value: bfloat16 [576, 3, 64], P(('row', 'col'))
- w_out: bfloat16 [9, 64, 576], P(None, None, ('row', 'col'))
- grad_next: float32 [32, 3, 576, 1536], P(('dp', 'row', 'col'))
Outputs:
- output 1: bfloat16 [1024, 64, 576], P(('dp', 'row', 'col'))
- output 2: float32 [3, 576, 1536], P(None, None, ('row', 'col'))
- output 3: float32 [32, 576, 9, 64], P(('dp', 'row', 'col'))
- output 4: float32 [32, 576, 3, 64], P(('dp', 'row', 'col'))
- output 5: float32 [32, 576, 3, 64], P(('dp', 'row', 'col'))
- output 6: float32 [32, 9, 64, 576], P(('dp', 'row', 'col'))
All inputs are finite; a program needn't handle non-finite values.
Results may differ from the reference program's by a relative error of at most 0.0105782.
Values are sent between devices in bfloat16 or wider.
A program may use at most 1 GiB of HBM per device.

```python
import jax
import jax.numpy as jnp
from jax import lax

NDEV = 32
TOKENS = 2048
SEQ = 64
D = 576
FF = 1536
HEADS = 9
KV_HEADS = 3
HEAD = 64
BATCH = TOKENS // SEQ
GROUP_SIZE = HEADS // KV_HEADS
HALF_DIM = HEAD // 2
SCORE_SCALE = HEAD ** -0.5


def setup_inputs(seed: int = 0) -> dict:
    key_list = jax.random.split(jax.random.key(seed), 7)
    act_shape = (NDEV * BATCH, SEQ, D)
    x_seq = jax.random.normal(key_list[0], act_shape, jnp.float32)
    dy_seq = jax.random.normal(key_list[1], act_shape, jnp.float32)
    w_query = jax.random.normal(key_list[2], (D, HEADS, HEAD), jnp.float32) * D ** -0.5
    w_key = jax.random.normal(key_list[3], (D, KV_HEADS, HEAD), jnp.float32) * D ** -0.5
    w_value = jax.random.normal(key_list[4], (D, KV_HEADS, HEAD), jnp.float32) * D ** -0.5
    w_out = jax.random.normal(key_list[5], (HEADS, HEAD, D), jnp.float32) * (HEADS * HEAD) ** -0.5
    grad_next = jax.random.normal(key_list[6], (NDEV, 3, D, FF), jnp.float32) * NDEV ** -0.5
    return {
        "x_seq": x_seq.astype(jnp.bfloat16),
        "dy_seq": dy_seq.astype(jnp.bfloat16),
        "w_query": w_query.astype(jnp.bfloat16),
        "w_key": w_key.astype(jnp.bfloat16),
        "w_value": w_value.astype(jnp.bfloat16),
        "w_out": w_out.astype(jnp.bfloat16),
        "grad_next": grad_next,
    }


def as_wide(arr_in):
    return arr_in.astype(jnp.float32)


def rope_tables():
    position = jnp.arange(SEQ, dtype=jnp.float32)
    inv_freq = 10000.0 ** (-jnp.arange(HALF_DIM, dtype=jnp.float32) * (2.0 / HEAD))
    angles = position[:, None] * inv_freq[None, :]
    return jnp.cos(angles)[:, None, :], jnp.sin(angles)[:, None, :]


def rope_apply(vals_in, cos_tab, sin_tab):
    first_half = vals_in[..., :HALF_DIM]
    second_half = vals_in[..., HALF_DIM:]
    return jnp.concatenate([first_half * cos_tab - second_half * sin_tab, second_half * cos_tab + first_half * sin_tab], axis=-1)


def rope_back(grads_in, cos_tab, sin_tab):
    first_half = grads_in[..., :HALF_DIM]
    second_half = grads_in[..., HALF_DIM:]
    return jnp.concatenate([first_half * cos_tab + second_half * sin_tab, second_half * cos_tab - first_half * sin_tab], axis=-1)


def device_backward(x_loc, dy_loc, w_query, w_key, w_value, w_out):
    cos_tab, sin_tab = rope_tables()
    x_wide = as_wide(x_loc)
    dy_wide = as_wide(dy_loc)
    query = rope_apply(jnp.einsum("bsm,mhd->bshd", x_wide, as_wide(w_query)), cos_tab, sin_tab).astype(jnp.bfloat16)
    key_rot = rope_apply(jnp.einsum("bsm,mnd->bsnd", x_wide, as_wide(w_key)), cos_tab, sin_tab).astype(jnp.bfloat16)
    value = jnp.einsum("bsm,mnd->bsnd", x_wide, as_wide(w_value)).astype(jnp.bfloat16)
    query_grp = query.reshape(BATCH, SEQ, KV_HEADS, GROUP_SIZE, HEAD)
    scores = jnp.einsum("bqngd,bknd->bngqk", as_wide(query_grp), as_wide(key_rot)) * SCORE_SCALE
    causal = jnp.arange(SEQ)[:, None] >= jnp.arange(SEQ)[None, :]
    attn_prob = jax.nn.softmax(jnp.where(causal, scores, -1e30), axis=-1)
    prob_low = attn_prob.astype(jnp.bfloat16)
    attn_out = jnp.einsum("bngqk,bknd->bqngd", as_wide(prob_low), as_wide(value)).astype(jnp.bfloat16).reshape(BATCH, SEQ, HEADS, HEAD)
    d_attn = jnp.einsum("bsm,hdm->bshd", dy_wide, as_wide(w_out)).astype(jnp.bfloat16).reshape(BATCH, SEQ, KV_HEADS, GROUP_SIZE, HEAD)
    d_prob = jnp.einsum("bqngd,bknd->bngqk", as_wide(d_attn), as_wide(value))
    d_value = jnp.einsum("bngqk,bqngd->bknd", as_wide(prob_low), as_wide(d_attn)).astype(jnp.bfloat16)
    row_delta = jnp.sum(attn_prob * d_prob, axis=-1, keepdims=True)
    d_scores = (attn_prob * (d_prob - row_delta) * SCORE_SCALE).astype(jnp.bfloat16)
    dq_rot = jnp.einsum("bngqk,bknd->bqngd", as_wide(d_scores), as_wide(key_rot)).reshape(BATCH, SEQ, HEADS, HEAD)
    dk_rot = jnp.einsum("bngqk,bqngd->bknd", as_wide(d_scores), as_wide(query_grp))
    d_query = rope_back(dq_rot, cos_tab, sin_tab).astype(jnp.bfloat16)
    d_key = rope_back(dk_rot, cos_tab, sin_tab).astype(jnp.bfloat16)
    grad_x = (jnp.einsum("bshd,mhd->bsm", as_wide(d_query), as_wide(w_query))
              + jnp.einsum("bsnd,mnd->bsm", as_wide(d_key), as_wide(w_key))
              + jnp.einsum("bsnd,mnd->bsm", as_wide(d_value), as_wide(w_value))).astype(jnp.bfloat16)
    grad_q = jnp.einsum("bsm,bshd->mhd", x_wide, as_wide(d_query))
    grad_k = jnp.einsum("bsm,bsnd->mnd", x_wide, as_wide(d_key))
    grad_v = jnp.einsum("bsm,bsnd->mnd", x_wide, as_wide(d_value))
    grad_o = jnp.einsum("bshd,bsm->hdm", as_wide(attn_out), dy_wide)
    return grad_x, grad_q, grad_k, grad_v, grad_o


def reference(x_seq, dy_seq, w_query, w_key, w_value, w_out, grad_next):
    x_dev = x_seq.reshape(NDEV, BATCH, SEQ, D)
    dy_dev = dy_seq.reshape(NDEV, BATCH, SEQ, D)
    grad_x, grad_q, grad_k, grad_v, grad_o = lax.map(
        lambda dev_pair: device_backward(dev_pair[0], dev_pair[1], w_query, w_key, w_value, w_out),
        (x_dev, dy_dev))
    dw_next = jnp.sum(grad_next.astype(jnp.bfloat16).astype(jnp.float32), axis=0)
    return grad_x.reshape(NDEV * BATCH, SEQ, D), dw_next, grad_q, grad_k, grad_v, grad_o
```

```python
import functools
import jax, jax.numpy as jnp, numpy as np
from jax import lax
from jax.experimental import pallas as pl
from jax.experimental.pallas import tpu as pltpu
from jax.sharding import PartitionSpec as P

T = 2048
D = 576
HD = 64
F32 = jnp.float32
BF = jnp.bfloat16
LOG2E = 1.4426950408889634


def rope_tables():
    pos = np.arange(64, dtype=np.float32)
    inv = np.float32(10000.0) ** (-np.arange(32, dtype=np.float32) * np.float32(2.0 / 64))
    ang = inv[:, None] * pos[None, :]
    cos, sin = np.cos(ang).astype(np.float32), np.sin(ang).astype(np.float32)
    return np.stack([np.tile(cos, (1, 4)), np.tile(sin, (1, 4))])


def nt(a, b):
    return lax.dot_general(a, b, (((1,), (1,)), ((), ())), preferred_element_type=F32)


def nn(a, b):
    return lax.dot_general(a, b, (((1,), (0,)), ((), ())), preferred_element_type=F32)


def tn(a, b):
    return lax.dot_general(a, b, (((0,), (0,)), ((), ())), preferred_element_type=F32)


def project(i, w, x, dy, tab, qkvT, doT, kl, vl):
    rows = pl.ds(pl.multiple_of(i * 256, 256), 256)
    cos, sin = tab[0], tab[1]
    raw = nt(w[0:960, :], x[rows, :])
    for h in range(12):
        a, b = raw[64 * h:64 * h + 32], raw[64 * h + 32:64 * h + 64]
        qkvT[64 * h:64 * h + 32, rows] = (a * cos - b * sin).astype(BF)
        qkvT[64 * h + 32:64 * h + 64, rows] = (b * cos + a * sin).astype(BF)
    qkvT[768:960, rows] = raw[768:960].astype(BF)
    doT[:, rows] = nt(w[960:1536, :], dy[rows, :]).astype(BF)
    for g in range(3):
        for src, dst in ((576, kl), (768, vl)):
            tr = qkvT[src + 64 * g:src + 64 * g + 64, rows].T
            for s in range(2):
                keys = pl.ds(pl.multiple_of(i * 128 + 64 * s, 64), 64)
                dst[g, keys, :] = jnp.concatenate([tr[128 * s:128 * s + 64], tr[128 * s + 64:128 * s + 128]], axis=1)


def attend(j, tab, qkvT, doT, kl, vl, oT, dqkvT):
    cols = pl.ds(pl.multiple_of(j * 128, 128), 128)
    keys = pl.ds(pl.multiple_of(j * 64, 64), 64)
    cos, sin = tab[0, :, 0:128], tab[1, :, 0:128]
    key_i = lax.broadcasted_iota(jnp.int32, (64, 384), 0)
    lane = lax.broadcasted_iota(jnp.int32, (64, 384), 1)
    causal = key_i <= lane % 64
    first = lane % 128 < 64
    zero = jnp.zeros((64, 384), BF)

    def blocks(v):
        return jnp.concatenate([jnp.where(first, v, zero), jnp.where(first, zero, v)], axis=0)

    for g in range(3):
        heads = [64 * (3 * g + r) for r in range(3)]
        q3 = jnp.concatenate([qkvT[h:h + 64, cols] for h in heads], axis=1)
        do3 = jnp.concatenate([doT[h:h + 64, cols] for h in heads], axis=1)
        kT = qkvT[576 + 64 * g:640 + 64 * g, cols]
        vT = qkvT[768 + 64 * g:832 + 64 * g, cols]
        s = nn(kl[g, keys, :], blocks(q3)) * (0.125 * LOG2E)
        dp = nn(vl[g, keys, :], blocks(do3))
        s = jnp.where(causal, s, -1e30)
        e = jnp.exp2(s - jnp.max(s, axis=0, keepdims=True))
        p = e * (1.0 / jnp.sum(e, axis=0, keepdims=True))
        delta = jnp.sum(p * dp, axis=0, keepdims=True)
        ds = (p * (dp - delta) * 0.125).astype(BF)
        pbd, dsbd = blocks(p.astype(BF)), blocks(ds)
        o = nn(vT, pbd).astype(BF)
        dq = nn(kT, dsbd)
        for r in range(3):
            h, c = heads[r], slice(128 * r, 128 * r + 128)
            oT[h:h + 64, cols] = o[:, c]
            a, b = dq[0:32, c], dq[32:64, c]
            dqkvT[h:h + 32, cols] = (a * cos + b * sin).astype(BF)
            dqkvT[h + 32:h + 64, cols] = (b * cos - a * sin).astype(BF)
        dqkvT[768 + 64 * g:832 + 64 * g, cols] = nt(do3, pbd).astype(BF)
        dk = nt(q3, dsbd)
        a, b = dk[0:32], dk[32:64]
        dqkvT[576 + 64 * g:608 + 64 * g, cols] = (a * cos + b * sin).astype(BF)
        dqkvT[608 + 64 * g:640 + 64 * g, cols] = (b * cos - a * sin).astype(BF)


def attn_kernel(x, dy, w, tab, dx, dwq, dwk, dwv, dwo, qkvT, doT, kl, vl, oT, dqkvT):
    @pl.loop(0, 8)
    def _(i):
        project(i, w, x, dy, tab, qkvT, doT, kl, vl)

    @pl.loop(0, 16)
    def _(j):
        attend(j, tab, qkvT, doT, kl, vl, oT, dqkvT)

    @pl.loop(0, 8)
    def _(i):
        rows = pl.ds(pl.multiple_of(i * 256, 256), 256)
        dx[rows, :] = tn(dqkvT[:, rows], w[0:960, :]).astype(BF)

    for lo in (0, 288):
        dwq[lo:lo + 288] = nn(dqkvT[lo:lo + 288, :], x[...])
        dwo[lo:lo + 288] = nn(oT[lo:lo + 288, :], dy[...])
    dkv = nn(dqkvT[576:960, :], x[...])
    dwk[...] = dkv[0:192]
    dwv[...] = dkv[192:384]


def attn(x, dy, w, tab):
    vm = pl.BlockSpec(memory_space=pltpu.VMEM)
    return pl.pallas_call(
        attn_kernel,
        out_shape=(jax.ShapeDtypeStruct((T, D), BF), jax.ShapeDtypeStruct((576, D), F32), jax.ShapeDtypeStruct((192, D), F32),
                   jax.ShapeDtypeStruct((192, D), F32), jax.ShapeDtypeStruct((576, D), F32)),
        in_specs=[vm] * 4, out_specs=[vm] * 5,
        scratch_shapes=[pltpu.VMEM((960, T), BF), pltpu.VMEM((576, T), BF), pltpu.VMEM((3, 1024, 128), BF),
                        pltpu.VMEM((3, 1024, 128), BF), pltpu.VMEM((576, T), BF), pltpu.VMEM((960, T), BF)],
        compiler_params=pltpu.CompilerParams(vmem_limit_bytes=60 * 2**20),
        cost_estimate=pl.CostEstimate(flops=40_000_000_000, bytes_accessed=20_000_000, transcendentals=1_000_000),
        name="attn_backward",
    )(x, dy, w, tab)


def solution(mesh):
    fsdp = ("row", "col")
    every = ("dp", "row", "col")

    def step(x_loc, dy_loc, wq, wk, wv, wo, g):
        slab = jnp.concatenate([jnp.transpose(wq, (1, 2, 0)).reshape(576, 72), jnp.transpose(wk, (1, 2, 0)).reshape(192, 72),
                                jnp.transpose(wv, (1, 2, 0)).reshape(192, 72), wo.reshape(576, 72)], axis=0)
        w = lax.all_gather(slab, fsdp, axis=1, tiled=True)
        group_sum = lax.psum_scatter(g.astype(BF), fsdp, scatter_dimension=3, tiled=True)
        dw_next = lax.psum(group_sum.astype(F32), "dp")[0]
        dx, dwq, dwk, dwv, dwo = attn(x_loc.reshape(T, D), dy_loc.reshape(T, D), w, jnp.asarray(rope_tables()))

        def head_first(a, n):
            return jnp.transpose(a.reshape(n, 64, D), (2, 0, 1))[None]

        return (dx.reshape(32, 64, D), dw_next, head_first(dwq, 9), head_first(dwk, 3), head_first(dwv, 3),
                dwo.reshape(1, 9, 64, D))

    return jax.shard_map(
        step, mesh=mesh,
        in_specs=(P(every), P(every), P(fsdp), P(fsdp), P(fsdp), P(None, None, fsdp), P(every)),
        out_specs=(P(every), P(None, None, fsdp), P(every), P(every), P(every), P(every)),
        check_vma=False)
```

```python
import functools
import jax, jax.numpy as jnp, numpy as np
from jax import lax
from jax.experimental import pallas as pl
from jax.experimental.pallas import tpu as pltpu
from jax.sharding import PartitionSpec as P

T = 2048
D = 576
HD = 64
F32 = jnp.float32
BF = jnp.bfloat16
LOG2E = 1.4426950408889634


def rope_tables():
    pos = np.arange(64, dtype=np.float32)
    inv = np.float32(10000.0) ** (-np.arange(32, dtype=np.float32) * np.float32(2.0 / 64))
    ang = inv[:, None] * pos[None, :]
    cos, sin = np.cos(ang).astype(np.float32), np.sin(ang).astype(np.float32)
    return np.stack([np.tile(cos, (1, 4)), np.tile(sin, (1, 4))])


def nt(a, b):
    return lax.dot_general(a, b, (((1,), (1,)), ((), ())), preferred_element_type=F32)


def nn(a, b):
    return lax.dot_general(a, b, (((1,), (0,)), ((), ())), preferred_element_type=F32)


def tn(a, b):
    return lax.dot_general(a, b, (((0,), (0,)), ((), ())), preferred_element_type=F32)


def project(i, w, x, dy, tab, qkvT, doT, kl, vl):
    rows = pl.ds(pl.multiple_of(i * 256, 256), 256)
    cos, sin = tab[0], tab[1]
    raw = nt(w[0:960, :], x[rows, :])
    for h in range(12):
        a, b = raw[64 * h:64 * h + 32], raw[64 * h + 32:64 * h + 64]
        qkvT[64 * h:64 * h + 32, rows] = (a * cos - b * sin).astype(BF)
        qkvT[64 * h + 32:64 * h + 64, rows] = (b * cos + a * sin).astype(BF)
    qkvT[768:960, rows] = raw[768:960].astype(BF)
    doT[:, rows] = nt(w[960:1536, :], dy[rows, :]).astype(BF)
    for g in range(3):
        for src, dst in ((576, kl), (768, vl)):
            tr = qkvT[src + 64 * g:src + 64 * g + 64, rows].T
            for s in range(2):
                keys = pl.ds(pl.multiple_of(i * 128 + 64 * s, 64), 64)
                dst[g, keys, :] = jnp.concatenate([tr[128 * s:128 * s + 64], tr[128 * s + 64:128 * s + 128]], axis=1)


def attend(j, tab, qkvT, doT, kl, vl, oT, dqkvT):
    cols = pl.ds(pl.multiple_of(j * 128, 128), 128)
    keys = pl.ds(pl.multiple_of(j * 64, 64), 64)
    cos, sin = tab[0, :, 0:128], tab[1, :, 0:128]
    key_i = lax.broadcasted_iota(jnp.int32, (64, 384), 0)
    lane = lax.broadcasted_iota(jnp.int32, (64, 384), 1)
    causal = key_i <= lane % 64
    first = lane % 128 < 64
    zero = jnp.zeros((64, 384), BF)

    def blocks(v):
        return jnp.concatenate([jnp.where(first, v, zero), jnp.where(first, zero, v)], axis=0)

    for g in range(3):
        heads = [64 * (3 * g + r) for r in range(3)]
        q3 = jnp.concatenate([qkvT[h:h + 64, cols] for h in heads], axis=1)
        do3 = jnp.concatenate([doT[h:h + 64, cols] for h in heads], axis=1)
        kT = qkvT[576 + 64 * g:640 + 64 * g, cols]
        vT = qkvT[768 + 64 * g:832 + 64 * g, cols]
        s = nn(kl[g, keys, :], blocks(q3)) * (0.125 * LOG2E)
        dp = nn(vl[g, keys, :], blocks(do3))
        s = jnp.where(causal, s, -1e30)
        e = jnp.exp2(s - jnp.max(s, axis=0, keepdims=True))
        p = e * (1.0 / jnp.sum(e, axis=0, keepdims=True))
        delta = jnp.sum(p * dp, axis=0, keepdims=True)
        ds = (p * (dp - delta) * 0.125).astype(BF)
        pbd, dsbd = blocks(p.astype(BF)), blocks(ds)
        o = nn(vT, pbd).astype(BF)
        dq = nn(kT, dsbd)
        for r in range(3):
            h, c = heads[r], slice(128 * r, 128 * r + 128)
            oT[h:h + 64, cols] = o[:, c]
            a, b = dq[0:32, c], dq[32:64, c]
            dqkvT[h:h + 32, cols] = (a * cos + b * sin).astype(BF)
            dqkvT[h + 32:h + 64, cols] = (b * cos - a * sin).astype(BF)
        dqkvT[768 + 64 * g:832 + 64 * g, cols] = nt(do3, pbd).astype(BF)
        dk = nt(q3, dsbd)
        a, b = dk[0:32], dk[32:64]
        dqkvT[576 + 64 * g:608 + 64 * g, cols] = (a * cos + b * sin).astype(BF)
        dqkvT[608 + 64 * g:640 + 64 * g, cols] = (b * cos - a * sin).astype(BF)


NP = 18
MESH = pl.DeviceIdType.MESH


def flip(bit, other):
    return 1 - other if bit else other


class Comm:
    def __init__(self, g, out, wl, pk, gf, gsh, d2d, u, r1, v, r2, gs, ze, za, zr, zf, outs, ssem, rsem, wss, wsr, gsem, osem):
        self.__dict__.update({k: val for k, val in locals().items() if k != "self"})
        self.z, self.y, self.col = lax.axis_index("dp"), lax.axis_index("row"), lax.axis_index("col")
        self.c, self.x = lax.rem(self.col, 2), lax.div(self.col, 2)
        self.sib = self.col + 1 - 2 * self.c
        self.xcol = (1 - self.x) * 2 + self.c
        self.yrow = 1 - self.y
        self.zp = self.z + 1 - 2 * lax.rem(self.z, 2)
        self.zm = 3 - self.z
        self.mid = (self.z == 1) | (self.z == 2)
        self.end = (self.z == 0) | (self.z == 3)
        self.sibling, self.xdev = (self.z, self.y, self.sib), (self.z, self.y, self.xcol)
        self.ydev, self.zdev, self.mdev = (self.z, self.yrow, self.col), (self.zp, self.y, self.col), (self.zm, self.y, self.col)

    def barrier(self):
        sem = pltpu.get_barrier_semaphore()
        for dev in (self.sibling, self.xdev, self.ydev, self.zdev):
            pl.semaphore_signal(sem, inc=1, device_id=dev, device_id_type=MESH)

        @pl.when(self.mid)
        def _():
            pl.semaphore_signal(sem, inc=1, device_id=self.mdev, device_id_type=MESH)

        pl.semaphore_wait(sem, 4 + lax.rem(lax.div(self.z + 1, 2), 2))

    def pack(self):
        mine = 4 * self.y + self.col
        self.pk[mine] = jnp.concatenate([self.wl[96 * j:96 * j + 96, :] for j in range(16)], axis=1)

    def unpack(self, w):
        for j in range(16):
            w[96 * j:96 * j + 96, :] = jnp.concatenate([self.pk[i, :, 72 * j:72 * j + 72] for i in range(8)], axis=1)

    def wcopy(self, n):
        me = 4 * self.y + self.col
        fx, fy, fd = 4 * self.y + self.xcol, 4 * self.yrow + self.col, 4 * self.yrow + self.xcol
        slab, lo, size, dev = (
            (me, 0, 48, self.xdev), (me, 48, 48, self.ydev), (me, 48, 48, self.xdev), (me, 0, 48, self.ydev),
            (me, 0, 96, self.sibling),
            (fx, 0, 48, self.ydev), (fy, 48, 48, self.xdev),
            (fx, 0, 96, self.sibling), (fy, 0, 96, self.sibling),
            (fd, 0, 48, self.sibling), (fd, 48, 48, self.sibling))[n]
        ref = self.pk.at[slab, pl.ds(lo, size), :]
        return pltpu.make_async_remote_copy(ref, ref, self.wss.at[n], self.wsr.at[n], device_id=dev, device_id_type=MESH)

    def load(self, p):
        k, r, slot = lax.div(p, 6), lax.rem(p, 6), lax.rem(p, 4)
        return [pltpu.make_async_copy(self.g.at[k, pl.ds(pl.multiple_of(288 * h + 48 * r, 48), 48), :],
                                      self.gf.at[slot, pl.ds(48 * h, 48), :], self.gsem.at[h, p]) for h in range(2)]

    def remote(self, n, src, dst, p, dev):
        return pltpu.make_async_remote_copy(src, dst, self.ssem.at[n, p], self.rsem.at[n, p], device_id=dev, device_id_type=MESH)

    def c0(self, p):
        return self.remote(0, self.gsh.at[p, 1], self.d2d.at[p], p, self.sibling)

    def c1(self, p):
        t = lax.rem(p, 2)
        dev = (self.z, self.y + t * (self.yrow - self.y), self.xcol + t * (self.col - self.xcol))
        return self.remote(1, self.u.at[p, 1], self.r1.at[p], p, dev)

    def c2(self, p):
        t = lax.rem(p, 2)
        dev = (self.z, self.yrow + t * (self.y - self.yrow), self.col + t * (self.xcol - self.col))
        return self.remote(2, self.v.at[p, 1], self.r2.at[p], p, dev)

    def c3(self, p):
        return self.remote(3, self.gs.at[p], self.ze.at[p], p, self.zdev)

    def c4(self, p):
        return self.remote(4, self.za.at[p], self.zr.at[p], p, self.mdev)

    def c5(self, p):
        return self.remote(5, self.zf.at[p], self.zr.at[p], p, self.zdev)

    def s1(self, p):
        for cp in self.load(p):
            cp.wait()
        slot = lax.rem(p, 4)
        for q in range(4):
            top = self.gf[slot, 0:48, 384 * q:384 * q + 384].astype(BF)
            bot = self.gf[slot, 48:96, 384 * q:384 * q + 384].astype(BF)
            for cc in range(2):
                lanes = slice(192 * cc, 192 * cc + 192)
                self.gsh[p, flip(cc, self.c), q] = jnp.concatenate([top[:, lanes], bot[:, lanes]], axis=1)
        self.c0(p).start()

        @pl.when(p + 4 < NP)
        def _():
            for cp in self.load(p + 4):
                cp.start()

    def s2(self, p):
        self.c0(p).wait_recv()
        t = lax.rem(p, 2)
        for yy in range(2):
            for xx in range(2):
                q = 2 * yy + xx
                fx, fy = flip(xx, self.x), flip(yy, self.y)
                self.u[p, fx + t * (fy - fx), yy + t * (xx - yy)] = self.gsh[p, 0, q] + self.d2d[p, q]
        self.c1(p).start()

    def s3(self, p):
        self.c1(p).wait_recv()
        t = lax.rem(p, 2)
        own = self.y + t * (self.x - self.y)
        for e in range(2):
            self.v[p, flip(e, own)] = self.u[p, 0, e] + self.r1[p, e]
        self.c2(p).start()

    def s4(self, p):
        self.c2(p).wait_recv()
        self.gs[p] = self.v[p, 0] + self.r2[p]

        @pl.when(self.end)
        def _():
            self.c3(p).start()

    def s5(self, p):
        @pl.when(self.mid)
        def _():
            self.c3(p).wait_recv()
            self.za[p] = self.gs[p].astype(F32) + self.ze[p].astype(F32)
            self.c4(p).start()

    def s6(self, p):
        @pl.when(self.mid)
        def _():
            self.c4(p).wait_recv()
            self.zf[p] = self.za[p] + self.zr[p]
            self.c5(p).start()

            @pl.when(lax.rem(p, 6) == 5)
            def _():
                self.emit(self.zf, lax.div(p, 6))

    def s7(self, p):
        @pl.when(self.end)
        def _():
            self.c5(p).wait_recv()

            @pl.when(lax.rem(p, 6) == 5)
            def _():
                self.emit(self.zr, lax.div(p, 6))

    def emit(self, buf, k):
        tr = buf[pl.ds(6 * k, 6)].reshape(288, 384).T
        self.outs[k] = jnp.concatenate([tr[0:192], tr[192:384]], axis=1)
        self.ocopy(k).start()

    def ocopy(self, k):
        return pltpu.make_async_copy(self.outs.at[k], self.out.at[k], self.osem.at[k])

    def step(self, t):
        for off, stage in zip(OFFSETS, (self.s1, self.s2, self.s3, self.s4, self.s5, self.s6, self.s7)):
            p = t - off

            @pl.when((p >= 0) & (p < NP))
            def _():
                stage(p)

    def drain(self):
        for n in range(11):
            self.wcopy(n).wait_send()

        @pl.loop(0, NP)
        def _(p):
            self.c0(p).wait_send()
            self.c1(p).wait_send()
            self.c2(p).wait_send()

            @pl.when(self.end)
            def _():
                self.c3(p).wait_send()

            @pl.when(self.mid)
            def _():
                self.c4(p).wait_send()
                self.c5(p).wait_send()

        for k in range(3):
            self.ocopy(k).wait()


OFFSETS = (0, 1, 3, 5, 6, 8, 10)


def kernel(x_h, dy_h, wq_h, wk_h, wv_h, wo_h, g, tab, dx_h, dwq_h, dwk_h, dwv_h, dwo_h, out,
           x, dy, w, qkvT, doT, kl, vl, oT, dqkvT, dx, dws, insem, outsem, *bufs):
    cm = Comm(g, out, *bufs)
    loads = [pltpu.make_async_copy(src, cm.wl.at[lo:lo + n, :], insem.at[i])
             for i, (src, lo, n) in enumerate(((wq_h, 0, 576), (wk_h, 576, 192), (wv_h, 768, 192), (wo_h, 960, 576)))]
    for cp in loads:
        cp.start()
    for p in range(4):
        for cp in cm.load(p):
            cp.start()
    acts = [pltpu.make_async_copy(x_h, x, insem.at[4]), pltpu.make_async_copy(dy_h, dy, insem.at[5])]
    for cp in acts:
        cp.start()
    cm.barrier()
    for cp in loads:
        cp.wait()
    cm.pack()
    for n in range(5):
        cm.wcopy(n).start()
    cm.step(0)
    cm.wcopy(0).wait_recv()
    cm.wcopy(5).start()
    cm.wcopy(1).wait_recv()
    cm.wcopy(6).start()
    cm.step(1)
    cm.wcopy(2).wait_recv()
    cm.wcopy(7).start()
    cm.wcopy(3).wait_recv()
    cm.wcopy(8).start()
    cm.step(2)
    cm.wcopy(5).wait_recv()
    cm.wcopy(9).start()
    cm.wcopy(6).wait_recv()
    cm.wcopy(10).start()
    for n in (4, 7, 8, 9, 10):
        cm.wcopy(n).wait_recv()
    cm.unpack(w)
    for cp in acts:
        cp.wait()

    @pl.loop(0, 8)
    def _(i):
        project(i, w, x, dy, tab, qkvT, doT, kl, vl)

        @pl.when(lax.rem(i, 2) == 1)
        def _():
            cm.step(3 + lax.div(i, 2))

    @pl.loop(0, 16)
    def _(j):
        attend(j, tab, qkvT, doT, kl, vl, oT, dqkvT)
        cm.step(7 + j)

    def dx_copy(i):
        rows = pl.ds(pl.multiple_of(i * 256, 256), 256)
        return pltpu.make_async_copy(dx.at[rows, :], dx_h.at[rows, :], outsem.at[i])

    @pl.loop(0, 8)
    def _(i):
        rows = pl.ds(pl.multiple_of(i * 256, 256), 256)
        dx[rows, :] = tn(dqkvT[:, rows], w[0:960, :]).astype(BF)
        dx_copy(i).start()

        @pl.when(lax.rem(i, 2) == 1)
        def _():
            cm.step(23 + lax.div(i, 2))

    def dw_copy(n):
        src, dst = ((dws.at[0:288], dwq_h.at[0:288]), (dws.at[288:576], dwq_h.at[288:576]), (dws.at[960:1248], dwo_h.at[0:288]),
                    (dws.at[1248:1536], dwo_h.at[288:576]), (dws.at[576:768], dwk_h), (dws.at[768:960], dwv_h))[n]
        return pltpu.make_async_copy(src, dst, outsem.at[8 + n])

    for h in range(2):
        lo = 288 * h
        dws[lo:lo + 288] = nn(dqkvT[lo:lo + 288, :], x[...])
        dw_copy(h).start()
        dws[960 + lo:1248 + lo] = nn(oT[lo:lo + 288, :], dy[...])
        dw_copy(2 + h).start()
    dws[576:960] = nn(dqkvT[576:960, :], x[...])
    dw_copy(4).start()
    dw_copy(5).start()

    @pl.loop(27, NP + OFFSETS[-1])
    def _(t):
        cm.step(t)

    for i in range(8):
        dx_copy(i).wait()
    for n in range(6):
        dw_copy(n).wait()
    cm.drain()


def backward(x, dy, wq, wk, wv, wo, g, tab):
    anyspace, vm = pl.BlockSpec(memory_space=pl.ANY), pl.BlockSpec(memory_space=pltpu.VMEM)

    def buf(*shape, dtype=BF):
        return pltpu.VMEM(shape, dtype)

    dma = pltpu.SemaphoreType.DMA
    return pl.pallas_call(
        kernel,
        out_shape=(jax.ShapeDtypeStruct((T, D), BF), jax.ShapeDtypeStruct((576, D), F32), jax.ShapeDtypeStruct((192, D), F32),
                   jax.ShapeDtypeStruct((192, D), F32), jax.ShapeDtypeStruct((576, D), F32),
                   jax.ShapeDtypeStruct((3, 192, D), F32)),
        in_specs=[anyspace] * 7 + [vm], out_specs=[anyspace] * 6,
        scratch_shapes=[
            buf(T, D), buf(T, D), buf(1536, D), buf(960, T), buf(576, T), buf(3, 1024, 128), buf(3, 1024, 128), buf(576, T),
            buf(960, T), buf(T, D), buf(1536, D, dtype=F32), dma((6,)), dma((14,)),
            buf(1536, 72), buf(8, 96, 1152), buf(4, 96, 1536, dtype=F32), buf(NP, 2, 4, 48, 384), buf(NP, 4, 48, 384),
            buf(NP, 2, 2, 48, 384), buf(NP, 2, 48, 384), buf(NP, 2, 48, 384), buf(NP, 48, 384), buf(NP, 48, 384),
            buf(NP, 48, 384), buf(NP, 48, 384, dtype=F32), buf(NP, 48, 384, dtype=F32), buf(NP, 48, 384, dtype=F32),
            buf(3, 192, D, dtype=F32), dma((6, NP)), dma((6, NP)), dma((11,)), dma((11,)), dma((2, NP)), dma((3,))],
        compiler_params=pltpu.CompilerParams(vmem_limit_bytes=67_000_000, collective_id=0, has_side_effects=True),
        name="attn_backward_and_sum",
    )(x, dy, wq, wk, wv, wo, g, tab)


def solution(mesh):
    fsdp = ("row", "col")
    every = ("dp", "row", "col")

    def step(x_loc, dy_loc, wq, wk, wv, wo, g):
        def rows_first(a):
            return jnp.transpose(a, (1, 2, 0)).reshape(-1, 72)

        dx, dwq, dwk, dwv, dwo, dw_next = backward(
            x_loc.reshape(T, D), dy_loc.reshape(T, D), rows_first(wq), rows_first(wk), rows_first(wv), wo.reshape(576, 72),
            g[0], jnp.asarray(rope_tables()))

        def head_first(a, n):
            return jnp.transpose(a.reshape(n, 64, D), (2, 0, 1))[None]

        return (dx.reshape(32, 64, D), jnp.transpose(dw_next, (0, 2, 1)), head_first(dwq, 9), head_first(dwk, 3),
                head_first(dwv, 3), dwo.reshape(1, 9, 64, D))

    return jax.shard_map(
        step, mesh=mesh,
        in_specs=(P(every), P(every), P(fsdp), P(fsdp), P(fsdp), P(None, None, fsdp), P(every)),
        out_specs=(P(every), P(None, None, fsdp), P(every), P(every), P(every), P(every)),
        check_vma=False)
```

```python
import functools
import jax, jax.numpy as jnp, numpy as np
from jax import lax
from jax.experimental import pallas as pl
from jax.experimental.pallas import tpu as pltpu
from jax.sharding import PartitionSpec as P

T = 2048
D = 576
HD = 64
F32 = jnp.float32
BF = jnp.bfloat16
LOG2E = 1.4426950408889634


def rope_tables():
    pos = np.arange(64, dtype=np.float32)
    inv = np.float32(10000.0) ** (-np.arange(32, dtype=np.float32) * np.float32(2.0 / 64))
    ang = inv[:, None] * pos[None, :]
    cos, sin = np.cos(ang).astype(np.float32), np.sin(ang).astype(np.float32)
    return np.stack([np.tile(cos, (1, 4)), np.tile(sin, (1, 4))])


def nt(a, b):
    return lax.dot_general(a, b, (((1,), (1,)), ((), ())), preferred_element_type=F32)


def nn(a, b):
    return lax.dot_general(a, b, (((1,), (0,)), ((), ())), preferred_element_type=F32)


def tn(a, b):
    return lax.dot_general(a, b, (((0,), (0,)), ((), ())), preferred_element_type=F32)


def project(i, w, x, dy, tab, qkvT, doT, kl, vl):
    rows = pl.ds(pl.multiple_of(i * 256, 256), 256)
    cos, sin = tab[0], tab[1]
    raw = nt(w[0:960, :], x[rows, :])
    for h in range(12):
        a, b = raw[64 * h:64 * h + 32], raw[64 * h + 32:64 * h + 64]
        qkvT[64 * h:64 * h + 32, rows] = (a * cos - b * sin).astype(BF)
        qkvT[64 * h + 32:64 * h + 64, rows] = (b * cos + a * sin).astype(BF)
    qkvT[768:960, rows] = raw[768:960].astype(BF)
    doT[:, rows] = nt(w[960:1536, :], dy[rows, :]).astype(BF)
    for g in range(3):
        for src, dst in ((576, kl), (768, vl)):
            tr = qkvT[src + 64 * g:src + 64 * g + 64, rows].T
            for s in range(2):
                keys = pl.ds(pl.multiple_of(i * 128 + 64 * s, 64), 64)
                dst[g, keys, :] = jnp.concatenate([tr[128 * s:128 * s + 64], tr[128 * s + 64:128 * s + 128]], axis=1)


def attend(j, tab, qkvT, doT, kl, vl, oT, dqkvT):
    cols = pl.ds(pl.multiple_of(j * 128, 128), 128)
    keys = pl.ds(pl.multiple_of(j * 64, 64), 64)
    cos, sin = tab[0, :, 0:128], tab[1, :, 0:128]
    key_i = lax.broadcasted_iota(jnp.int32, (64, 384), 0)
    lane = lax.broadcasted_iota(jnp.int32, (64, 384), 1)
    causal = key_i <= lane % 64
    first = lane % 128 < 64
    zero = jnp.zeros((64, 384), BF)

    def blocks(v):
        return jnp.concatenate([jnp.where(first, v, zero), jnp.where(first, zero, v)], axis=0)

    for g in range(3):
        heads = [64 * (3 * g + r) for r in range(3)]
        q3 = jnp.concatenate([qkvT[h:h + 64, cols] for h in heads], axis=1)
        do3 = jnp.concatenate([doT[h:h + 64, cols] for h in heads], axis=1)
        kT = qkvT[576 + 64 * g:640 + 64 * g, cols]
        vT = qkvT[768 + 64 * g:832 + 64 * g, cols]
        s = nn(kl[g, keys, :], blocks(q3)) * (0.125 * LOG2E)
        dp = nn(vl[g, keys, :], blocks(do3))
        s = jnp.where(causal, s, -1e30)
        e = jnp.exp2(s - jnp.max(s, axis=0, keepdims=True))
        p = e * (1.0 / jnp.sum(e, axis=0, keepdims=True))
        delta = jnp.sum(p * dp, axis=0, keepdims=True)
        ds = (p * (dp - delta) * 0.125).astype(BF)
        pbd, dsbd = blocks(p.astype(BF)), blocks(ds)
        o = nn(vT, pbd).astype(BF)
        dq = nn(kT, dsbd)
        for r in range(3):
            h, c = heads[r], slice(128 * r, 128 * r + 128)
            oT[h:h + 64, cols] = o[:, c]
            a, b = dq[0:32, c], dq[32:64, c]
            dqkvT[h:h + 32, cols] = (a * cos + b * sin).astype(BF)
            dqkvT[h + 32:h + 64, cols] = (b * cos - a * sin).astype(BF)
        dqkvT[768 + 64 * g:832 + 64 * g, cols] = nt(do3, pbd).astype(BF)
        dk = nt(q3, dsbd)
        a, b = dk[0:32], dk[32:64]
        dqkvT[576 + 64 * g:608 + 64 * g, cols] = (a * cos + b * sin).astype(BF)
        dqkvT[608 + 64 * g:640 + 64 * g, cols] = (b * cos - a * sin).astype(BF)


NP = 18
MESH = pl.DeviceIdType.MESH


def flip(bit, other):
    return 1 - other if bit else other


class Comm:
    def __init__(self, g, out, wl, pk, gf, gsh, d2d, u, r1, v, r2, gs, ze, za, zr, zf, ssem, rsem, wss, wsr, gsem):
        self.__dict__.update({k: val for k, val in locals().items() if k != "self"})
        self.z, self.y, self.col = lax.axis_index("dp"), lax.axis_index("row"), lax.axis_index("col")
        self.c, self.x = lax.rem(self.col, 2), lax.div(self.col, 2)
        self.sib = self.col + 1 - 2 * self.c
        self.xcol = (1 - self.x) * 2 + self.c
        self.yrow = 1 - self.y
        self.zp = self.z + 1 - 2 * lax.rem(self.z, 2)
        self.zm = 3 - self.z
        self.mid = (self.z == 1) | (self.z == 2)
        self.end = (self.z == 0) | (self.z == 3)
        self.sibling, self.xdev = (self.z, self.y, self.sib), (self.z, self.y, self.xcol)
        self.ydev, self.zdev, self.mdev = (self.z, self.yrow, self.col), (self.zp, self.y, self.col), (self.zm, self.y, self.col)

    def barrier(self):
        sem = pltpu.get_barrier_semaphore()
        for dev in (self.sibling, self.xdev, self.ydev, self.zdev):
            pl.semaphore_signal(sem, inc=1, device_id=dev, device_id_type=MESH)

        @pl.when(self.mid)
        def _():
            pl.semaphore_signal(sem, inc=1, device_id=self.mdev, device_id_type=MESH)

        pl.semaphore_wait(sem, 4 + lax.rem(lax.div(self.z + 1, 2), 2))

    def pack(self):
        mine = 4 * self.y + self.col
        self.pk[mine] = jnp.concatenate([self.wl[96 * j:96 * j + 96, :] for j in range(16)], axis=1)

    def unpack(self, w):
        for j in range(16):
            w[96 * j:96 * j + 96, :] = jnp.concatenate([self.pk[i, :, 72 * j:72 * j + 72] for i in range(8)], axis=1)

    def wcopy(self, n):
        me = 4 * self.y + self.col
        fx, fy, fd = 4 * self.y + self.xcol, 4 * self.yrow + self.col, 4 * self.yrow + self.xcol
        slab, lo, size, dev = (
            (me, 0, 48, self.xdev), (me, 48, 48, self.ydev), (me, 48, 48, self.xdev), (me, 0, 48, self.ydev),
            (me, 0, 96, self.sibling),
            (fx, 0, 48, self.ydev), (fy, 48, 48, self.xdev),
            (fx, 0, 96, self.sibling), (fy, 0, 96, self.sibling),
            (fd, 0, 48, self.sibling), (fd, 48, 48, self.sibling))[n]
        ref = self.pk.at[slab, pl.ds(lo, size), :]
        return pltpu.make_async_remote_copy(ref, ref, self.wss.at[n], self.wsr.at[n], device_id=dev, device_id_type=MESH)

    def load(self, p):
        k, r, slot = lax.div(p, 6), lax.rem(p, 6), lax.rem(p, 4)
        return [pltpu.make_async_copy(self.g.at[k, pl.ds(pl.multiple_of(288 * h + 48 * r, 48), 48), :],
                                      self.gf.at[slot, pl.ds(48 * h, 48), :], self.gsem.at[h, p]) for h in range(2)]

    def remote(self, n, src, dst, p, dev):
        return pltpu.make_async_remote_copy(src, dst, self.ssem.at[n, p], self.rsem.at[n, p], device_id=dev, device_id_type=MESH)

    def c0(self, p):
        return self.remote(0, self.gsh.at[p, 1], self.d2d.at[p], p, self.sibling)

    def c1(self, p):
        t = lax.rem(p, 2)
        dev = (self.z, self.y + t * (self.yrow - self.y), self.xcol + t * (self.col - self.xcol))
        return self.remote(1, self.u.at[p, 1], self.r1.at[p], p, dev)

    def c2(self, p):
        t = lax.rem(p, 2)
        dev = (self.z, self.yrow + t * (self.y - self.yrow), self.col + t * (self.xcol - self.col))
        return self.remote(2, self.v.at[p, 1], self.r2.at[p], p, dev)

    def c3(self, p):
        return self.remote(3, self.gs.at[p], self.ze.at[p], p, self.zdev)

    def c4(self, p):
        return self.remote(4, self.za.at[p], self.zr.at[p], p, self.mdev)

    def c5(self, p):
        return self.remote(5, self.zf.at[p], self.zr.at[p], p, self.zdev)

    def s1(self, p):
        for cp in self.load(p):
            cp.wait()
        slot = lax.rem(p, 4)
        for q in range(4):
            top = self.gf[slot, 0:48, 384 * q:384 * q + 384].astype(BF)
            bot = self.gf[slot, 48:96, 384 * q:384 * q + 384].astype(BF)
            for cc in range(2):
                lanes = slice(192 * cc, 192 * cc + 192)
                self.gsh[p, flip(cc, self.c), q] = jnp.concatenate([top[:, lanes], bot[:, lanes]], axis=1)
        self.c0(p).start()

        @pl.when(p + 4 < NP)
        def _():
            for cp in self.load(p + 4):
                cp.start()

    def convert(self, lo, hi):
        @pl.loop(lo, hi)
        def _(p):
            self.s1(p)

    def forward(self, got, send):
        self.wcopy(got).wait_recv()
        self.wcopy(send).start()

    def s2(self, p):
        self.c0(p).wait_recv()
        t = lax.rem(p, 2)
        for yy in range(2):
            for xx in range(2):
                q = 2 * yy + xx
                fx, fy = flip(xx, self.x), flip(yy, self.y)
                self.u[p, fx + t * (fy - fx), yy + t * (xx - yy)] = self.gsh[p, 0, q] + self.d2d[p, q]
        self.c1(p).start()

    def s3(self, p):
        self.c1(p).wait_recv()
        t = lax.rem(p, 2)
        own = self.y + t * (self.x - self.y)
        for e in range(2):
            self.v[p, flip(e, own)] = self.u[p, 0, e] + self.r1[p, e]
        self.c2(p).start()

    def s4(self, p):
        self.c2(p).wait_recv()
        self.gs[p] = self.v[p, 0] + self.r2[p]

        @pl.when(self.end)
        def _():
            self.c3(p).start()

    def s5(self, p):
        @pl.when(self.mid)
        def _():
            self.c3(p).wait_recv()
            self.za[p] = self.gs[p].astype(F32) + self.ze[p].astype(F32)
            self.c4(p).start()

    def s6(self, p):
        @pl.when(self.mid)
        def _():
            self.c4(p).wait_recv()
            self.zf[p] = self.za[p] + self.zr[p]
            self.c5(p).start()

            @pl.when(lax.rem(p, 6) == 5)
            def _():
                self.emit(self.zf, lax.div(p, 6))

    def s7(self, p):
        @pl.when(self.end)
        def _():
            self.c5(p).wait_recv()

            @pl.when(lax.rem(p, 6) == 5)
            def _():
                self.emit(self.zr, lax.div(p, 6))

    def emit(self, buf, k):
        tr = buf[pl.ds(6 * k, 6)].reshape(288, 384).T
        self.out[k] = jnp.concatenate([tr[0:192], tr[192:384]], axis=1)

    def step(self, t):
        for off, stage in zip(OFFSETS, (self.s2, self.s3, self.s4, self.s5, self.s6, self.s7)):
            p = t - off

            @pl.when((p >= 0) & (p < NP))
            def _():
                stage(p)

    def drain(self):
        for n in range(11):
            self.wcopy(n).wait_send()

        @pl.loop(0, NP)
        def _(p):
            self.c0(p).wait_send()
            self.c1(p).wait_send()
            self.c2(p).wait_send()

            @pl.when(self.end)
            def _():
                self.c3(p).wait_send()

            @pl.when(self.mid)
            def _():
                self.c4(p).wait_send()
                self.c5(p).wait_send()


OFFSETS = (0, 3, 5, 7, 10, 13)


def kernel(x_h, dy_h, wq_h, wk_h, wv_h, wo_h, g, tab, dx, dwq, dwk, dwv, dwo, out,
           x, dy, w, qkvT, doT, kl, vl, oT, dqkvT, insem, *bufs):
    cm = Comm(g, out, *bufs)
    loads = [pltpu.make_async_copy(src, cm.wl.at[lo:lo + n, :], insem.at[i])
             for i, (src, lo, n) in enumerate(((wq_h, 0, 576), (wk_h, 576, 192), (wv_h, 768, 192), (wo_h, 960, 576)))]
    for cp in loads:
        cp.start()
    for p in range(4):
        for cp in cm.load(p):
            cp.start()
    acts = [pltpu.make_async_copy(x_h, x, insem.at[4]), pltpu.make_async_copy(dy_h, dy, insem.at[5])]
    for cp in acts:
        cp.start()
    cm.barrier()
    for cp in loads:
        cp.wait()
    cm.pack()
    for n in range(5):
        cm.wcopy(n).start()
    cm.convert(0, 3)
    cm.step(0)
    cm.convert(3, 5)
    cm.step(1)
    cm.forward(0, 5)
    cm.forward(1, 6)
    cm.convert(5, 9)
    cm.step(2)
    cm.forward(2, 7)
    cm.forward(3, 8)
    cm.convert(9, 13)
    cm.step(3)
    cm.convert(13, NP)
    cm.step(4)
    cm.forward(5, 9)
    cm.forward(6, 10)
    cm.step(5)
    for n in (4, 7, 8, 9, 10):
        cm.wcopy(n).wait_recv()
    cm.unpack(w)
    for cp in acts:
        cp.wait()

    def some(i, first, period, of):
        @pl.when(lax.rem(i, period) < of)
        def _():
            cm.step(first + of * lax.div(i, period) + lax.rem(i, period))

    @pl.loop(0, 8)
    def _(i):
        project(i, w, x, dy, tab, qkvT, doT, kl, vl)
        some(i, 6, 3, 2)

    @pl.loop(0, 16)
    def _(j):
        attend(j, tab, qkvT, doT, kl, vl, oT, dqkvT)
        some(j, 12, 3, 2)

    @pl.loop(0, 8)
    def _(i):
        rows = pl.ds(pl.multiple_of(i * 256, 256), 256)
        dx[rows, :] = tn(dqkvT[:, rows], w[0:960, :]).astype(BF)
        some(i, 23, 2, 1)

    @pl.loop(0, 2)
    def _(h):
        rows = pl.ds(pl.multiple_of(288 * h, 288), 288)
        dwq[rows, :] = nn(dqkvT[rows, :], x[...])
        dwo[rows, :] = nn(oT[rows, :], dy[...])
        cm.step(27 + h)

    dkv = nn(dqkvT[576:960, :], x[...])
    dwk[...] = dkv[0:192]
    dwv[...] = dkv[192:384]

    @pl.loop(29, NP + OFFSETS[-1])
    def _(t):
        cm.step(t)

    cm.drain()


def backward(x, dy, wq, wk, wv, wo, g, tab):
    hbm, vm = pl.BlockSpec(memory_space=pltpu.HBM), pl.BlockSpec(memory_space=pltpu.VMEM)

    def buf(*shape, dtype=BF):
        return pltpu.VMEM(shape, dtype)

    dma = pltpu.SemaphoreType.DMA
    return pl.pallas_call(
        kernel,
        out_shape=(buf(T, D), buf(576, D, dtype=F32), buf(192, D, dtype=F32), buf(192, D, dtype=F32), buf(576, D, dtype=F32),
                   buf(3, 192, D, dtype=F32)),
        in_specs=[hbm] * 7 + [vm], out_specs=[vm] * 6,
        scratch_shapes=[
            buf(T, D), buf(T, D), buf(1536, D), buf(960, T), buf(576, T), buf(3, 1024, 128), buf(3, 1024, 128), buf(576, T),
            buf(960, T), dma((6,)),
            buf(1536, 72), buf(8, 96, 1152), buf(4, 96, 1536, dtype=F32), buf(NP, 2, 4, 48, 384), buf(NP, 4, 48, 384),
            buf(NP, 2, 2, 48, 384), buf(NP, 2, 48, 384), buf(NP, 2, 48, 384), buf(NP, 48, 384), buf(NP, 48, 384),
            buf(NP, 48, 384), buf(NP, 48, 384, dtype=F32), buf(NP, 48, 384, dtype=F32), buf(NP, 48, 384, dtype=F32),
            dma((6, NP)), dma((6, NP)), dma((11,)), dma((11,)), dma((2, NP))],
        compiler_params=pltpu.CompilerParams(vmem_limit_bytes=50 * 2**20, collective_id=0, has_side_effects=True),
        name="attn_backward_and_sum",
    )(x, dy, wq, wk, wv, wo, g, tab)


def write_kernel(*refs):
    n = len(refs) // 2
    sem = refs[-1]
    copies = [pltpu.make_async_copy(refs[i], refs[n + i], sem.at[i]) for i in range(n)]
    for cp in copies:
        cp.start()
    for cp in copies:
        cp.wait()


def write_out(arrays):
    return pl.pallas_call(
        write_kernel, out_shape=[jax.ShapeDtypeStruct(a.shape, a.dtype) for a in arrays],
        in_specs=[pl.BlockSpec(memory_space=pltpu.VMEM)] * len(arrays),
        out_specs=[pl.BlockSpec(memory_space=pltpu.HBM)] * len(arrays),
        scratch_shapes=[pltpu.SemaphoreType.DMA((len(arrays),))],
        compiler_params=pltpu.CompilerParams(vmem_limit_bytes=2**20), name="write_out")(*arrays)


def solution(mesh):
    fsdp = ("row", "col")
    every = ("dp", "row", "col")

    def step(x_loc, dy_loc, wq, wk, wv, wo, g):
        def rows_first(a):
            return jnp.transpose(a, (1, 2, 0)).reshape(-1, 72)

        dx, dwq, dwk, dwv, dwo, dw_next = write_out(backward(
            x_loc.reshape(T, D), dy_loc.reshape(T, D), rows_first(wq), rows_first(wk), rows_first(wv), wo.reshape(576, 72),
            g[0], jnp.asarray(rope_tables())))

        def head_first(a, n):
            return jnp.transpose(a.reshape(n, 64, D), (2, 0, 1))[None]

        return (dx.reshape(32, 64, D), jnp.transpose(dw_next, (0, 2, 1)), head_first(dwq, 9), head_first(dwk, 3),
                head_first(dwv, 3), dwo.reshape(1, 9, 64, D))

    return jax.shard_map(
        step, mesh=mesh,
        in_specs=(P(every), P(every), P(fsdp), P(fsdp), P(fsdp), P(None, None, fsdp), P(every)),
        out_specs=(P(every), P(None, None, fsdp), P(every), P(every), P(every), P(every)),
        check_vma=False)
```

```python
import functools
import jax, jax.numpy as jnp, numpy as np
from jax import lax
from jax.experimental import pallas as pl
from jax.experimental.pallas import tpu as pltpu
from jax.sharding import PartitionSpec as P

T = 2048
D = 576
HD = 64
F32 = jnp.float32
BF = jnp.bfloat16
LOG2E = 1.4426950408889634


def rope_tables():
    pos = np.arange(64, dtype=np.float32)
    inv = np.float32(10000.0) ** (-np.arange(32, dtype=np.float32) * np.float32(2.0 / 64))
    ang = inv[:, None] * pos[None, :]
    cos, sin = np.cos(ang).astype(np.float32), np.sin(ang).astype(np.float32)
    return np.stack([np.tile(cos, (1, 4)), np.tile(sin, (1, 4))])


def nt(a, b):
    return lax.dot_general(a, b, (((1,), (1,)), ((), ())), preferred_element_type=F32)


def nn(a, b):
    return lax.dot_general(a, b, (((1,), (0,)), ((), ())), preferred_element_type=F32)


def tn(a, b):
    return lax.dot_general(a, b, (((0,), (0,)), ((), ())), preferred_element_type=F32)


def project(i, w, x, dy, tab, qkvT, doT, kl, vl):
    rows = pl.ds(pl.multiple_of(i * 256, 256), 256)
    cos, sin = tab[0], tab[1]
    raw = nt(w[0:960, :], x[rows, :])
    for h in range(12):
        a, b = raw[64 * h:64 * h + 32], raw[64 * h + 32:64 * h + 64]
        qkvT[64 * h:64 * h + 32, rows] = (a * cos - b * sin).astype(BF)
        qkvT[64 * h + 32:64 * h + 64, rows] = (b * cos + a * sin).astype(BF)
    qkvT[768:960, rows] = raw[768:960].astype(BF)
    doT[:, rows] = nt(w[960:1536, :], dy[rows, :]).astype(BF)
    for g in range(3):
        for src, dst in ((576, kl), (768, vl)):
            tr = qkvT[src + 64 * g:src + 64 * g + 64, rows].T
            for s in range(2):
                keys = pl.ds(pl.multiple_of(i * 128 + 64 * s, 64), 64)
                dst[g, keys, :] = jnp.concatenate([tr[128 * s:128 * s + 64], tr[128 * s + 64:128 * s + 128]], axis=1)


def attend(j, tab, qkvT, doT, kl, vl, oT, dqkvT):
    cols = pl.ds(pl.multiple_of(j * 128, 128), 128)
    keys = pl.ds(pl.multiple_of(j * 64, 64), 64)
    cos, sin = tab[0, :, 0:128], tab[1, :, 0:128]
    key_i = lax.broadcasted_iota(jnp.int32, (64, 384), 0)
    lane = lax.broadcasted_iota(jnp.int32, (64, 384), 1)
    causal = key_i <= lane % 64
    first = lane % 128 < 64
    zero = jnp.zeros((64, 384), BF)

    def blocks(v):
        return jnp.concatenate([jnp.where(first, v, zero), jnp.where(first, zero, v)], axis=0)

    loaded = []
    for g in range(3):
        heads = [64 * (3 * g + r) for r in range(3)]
        q3 = jnp.concatenate([qkvT[h:h + 64, cols] for h in heads], axis=1)
        do3 = jnp.concatenate([doT[h:h + 64, cols] for h in heads], axis=1)
        loaded.append((heads, q3, do3, nn(kl[g, keys, :], blocks(q3)), nn(vl[g, keys, :], blocks(do3))))
    soft = []
    for g in range(3):
        heads, q3, do3, s, dp = loaded[g]
        s = jnp.where(causal, s * (0.125 * LOG2E), -1e30)
        e = jnp.exp2(s - jnp.max(s, axis=0, keepdims=True))
        p = e * (1.0 / jnp.sum(e, axis=0, keepdims=True))
        delta = jnp.sum(p * dp, axis=0, keepdims=True)
        ds = (p * (dp - delta) * 0.125).astype(BF)
        soft.append((blocks(p.astype(BF)), blocks(ds)))
    for g in range(3):
        heads, q3, do3, s, dp = loaded[g]
        kT = qkvT[576 + 64 * g:640 + 64 * g, cols]
        vT = qkvT[768 + 64 * g:832 + 64 * g, cols]
        pbd, dsbd = soft[g]
        o = nn(vT, pbd).astype(BF)
        dq = nn(kT, dsbd)
        for r in range(3):
            h, c = heads[r], slice(128 * r, 128 * r + 128)
            oT[h:h + 64, cols] = o[:, c]
            a, b = dq[0:32, c], dq[32:64, c]
            dqkvT[h:h + 32, cols] = (a * cos + b * sin).astype(BF)
            dqkvT[h + 32:h + 64, cols] = (b * cos - a * sin).astype(BF)
        dqkvT[768 + 64 * g:832 + 64 * g, cols] = nt(do3, pbd).astype(BF)
        dk = nt(q3, dsbd)
        a, b = dk[0:32], dk[32:64]
        dqkvT[576 + 64 * g:608 + 64 * g, cols] = (a * cos + b * sin).astype(BF)
        dqkvT[608 + 64 * g:640 + 64 * g, cols] = (b * cos - a * sin).astype(BF)


NP = 18
MESH = pl.DeviceIdType.MESH


def flip(bit, other):
    return 1 - other if bit else other


class Comm:
    def __init__(self, g, out, wl, pk, gf, gsh, d2d, u, r1, v, r2, gs, ze, za, zr, zf, ssem, rsem, wss, wsr, gsem):
        self.__dict__.update({k: val for k, val in locals().items() if k != "self"})
        self.z, self.y, self.col = lax.axis_index("dp"), lax.axis_index("row"), lax.axis_index("col")
        self.c, self.x = lax.rem(self.col, 2), lax.div(self.col, 2)
        self.sib = self.col + 1 - 2 * self.c
        self.xcol = (1 - self.x) * 2 + self.c
        self.yrow = 1 - self.y
        self.zp = self.z + 1 - 2 * lax.rem(self.z, 2)
        self.zm = 3 - self.z
        self.mid = (self.z == 1) | (self.z == 2)
        self.end = (self.z == 0) | (self.z == 3)
        self.sibling, self.xdev = (self.z, self.y, self.sib), (self.z, self.y, self.xcol)
        self.ydev, self.zdev, self.mdev = (self.z, self.yrow, self.col), (self.zp, self.y, self.col), (self.zm, self.y, self.col)

    def barrier(self):
        sem = pltpu.get_barrier_semaphore()
        for dev in (self.sibling, self.xdev, self.ydev, self.zdev):
            pl.semaphore_signal(sem, inc=1, device_id=dev, device_id_type=MESH)

        @pl.when(self.mid)
        def _():
            pl.semaphore_signal(sem, inc=1, device_id=self.mdev, device_id_type=MESH)

        pl.semaphore_wait(sem, 4 + lax.rem(lax.div(self.z + 1, 2), 2))

    def pack(self):
        mine = 4 * self.y + self.col
        self.pk[mine] = jnp.concatenate([self.wl[96 * j:96 * j + 96, :] for j in range(16)], axis=1)

    def unpack(self, w):
        for j in range(16):
            w[96 * j:96 * j + 96, :] = jnp.concatenate([self.pk[i, :, 72 * j:72 * j + 72] for i in range(8)], axis=1)

    def wcopy(self, n):
        me = 4 * self.y + self.col
        fx, fy, fd = 4 * self.y + self.xcol, 4 * self.yrow + self.col, 4 * self.yrow + self.xcol
        slab, lo, size, dev = (
            (me, 0, 48, self.xdev), (me, 48, 48, self.ydev), (me, 48, 48, self.xdev), (me, 0, 48, self.ydev),
            (me, 0, 96, self.sibling),
            (fx, 0, 48, self.ydev), (fy, 48, 48, self.xdev),
            (fx, 0, 96, self.sibling), (fy, 0, 96, self.sibling),
            (fd, 0, 48, self.sibling), (fd, 48, 48, self.sibling))[n]
        ref = self.pk.at[slab, pl.ds(lo, size), :]
        return pltpu.make_async_remote_copy(ref, ref, self.wss.at[n], self.wsr.at[n], device_id=dev, device_id_type=MESH)

    def load(self, p):
        k, r, slot = lax.div(p, 6), lax.rem(p, 6), lax.rem(p, 4)
        return [pltpu.make_async_copy(self.g.at[k, pl.ds(pl.multiple_of(288 * h + 48 * r, 48), 48), :],
                                      self.gf.at[slot, pl.ds(48 * h, 48), :], self.gsem.at[h, p]) for h in range(2)]

    def remote(self, n, src, dst, p, dev):
        return pltpu.make_async_remote_copy(src, dst, self.ssem.at[n, p], self.rsem.at[n, p], device_id=dev, device_id_type=MESH)

    def c0(self, p):
        return self.remote(0, self.gsh.at[p, 1], self.d2d.at[p], p, self.sibling)

    def c1(self, p):
        t = lax.rem(p, 2)
        dev = (self.z, self.y + t * (self.yrow - self.y), self.xcol + t * (self.col - self.xcol))
        return self.remote(1, self.u.at[p, 1], self.r1.at[p], p, dev)

    def c2(self, p):
        t = lax.rem(p, 2)
        dev = (self.z, self.yrow + t * (self.y - self.yrow), self.col + t * (self.xcol - self.col))
        return self.remote(2, self.v.at[p, 1], self.r2.at[p], p, dev)

    def c3(self, p):
        return self.remote(3, self.gs.at[p], self.ze.at[p], p, self.zdev)

    def c4(self, p):
        return self.remote(4, self.za.at[p], self.zr.at[p], p, self.mdev)

    def c5(self, p):
        return self.remote(5, self.zf.at[p], self.zr.at[p], p, self.zdev)

    def s1(self, p):
        for cp in self.load(p):
            cp.wait()
        slot = lax.rem(p, 4)
        for q in range(4):
            top = self.gf[slot, 0:48, 384 * q:384 * q + 384].astype(BF)
            bot = self.gf[slot, 48:96, 384 * q:384 * q + 384].astype(BF)
            for cc in range(2):
                lanes = slice(192 * cc, 192 * cc + 192)
                self.gsh[p, flip(cc, self.c), q] = jnp.concatenate([top[:, lanes], bot[:, lanes]], axis=1)
        self.c0(p).start()

        @pl.when(p + 4 < NP)
        def _():
            for cp in self.load(p + 4):
                cp.start()

    def convert(self, lo, hi):
        @pl.loop(lo, hi)
        def _(p):
            self.s1(p)

    def forward(self, got, send):
        self.wcopy(got).wait_recv()
        self.wcopy(send).start()

    def s2(self, p):
        self.c0(p).wait_recv()
        t = lax.rem(p, 2)
        for yy in range(2):
            for xx in range(2):
                q = 2 * yy + xx
                fx, fy = flip(xx, self.x), flip(yy, self.y)
                self.u[p, fx + t * (fy - fx), yy + t * (xx - yy)] = self.gsh[p, 0, q] + self.d2d[p, q]
        self.c1(p).start()

    def s3(self, p):
        self.c1(p).wait_recv()
        t = lax.rem(p, 2)
        own = self.y + t * (self.x - self.y)
        for e in range(2):
            self.v[p, flip(e, own)] = self.u[p, 0, e] + self.r1[p, e]
        self.c2(p).start()

    def s4(self, p):
        self.c2(p).wait_recv()
        self.gs[p] = self.v[p, 0] + self.r2[p]

        @pl.when(self.end)
        def _():
            self.c3(p).start()

    def s5(self, p):
        @pl.when(self.mid)
        def _():
            self.c3(p).wait_recv()
            self.za[p] = self.gs[p].astype(F32) + self.ze[p].astype(F32)
            self.c4(p).start()

    def s6(self, p):
        @pl.when(self.mid)
        def _():
            self.c4(p).wait_recv()
            self.zf[p] = self.za[p] + self.zr[p]
            self.c5(p).start()

            @pl.when(lax.rem(p, 6) == 5)
            def _():
                self.emit(self.zf, lax.div(p, 6))

    def s7(self, p):
        @pl.when(self.end)
        def _():
            self.c5(p).wait_recv()

            @pl.when(lax.rem(p, 6) == 5)
            def _():
                self.emit(self.zr, lax.div(p, 6))

    def emit(self, buf, k):
        tr = buf[pl.ds(6 * k, 6)].reshape(288, 384).T
        self.out[k] = jnp.concatenate([tr[0:192], tr[192:384]], axis=1)

    def slot(self, now, length):
        for k in (7, 6, 5, 4, 3, 2):
            first = now - START[k] + 10 * PACE
            p = lax.div(first, PACE) - 10

            @pl.when((lax.div(first + length, PACE) - 10 > p) & (p >= AHEAD[k]) & (p < NP))
            def _():
                getattr(self, f"s{k}")(p)

    def run(self, k, lo, hi):
        @pl.loop(lo, hi)
        def _(p):
            getattr(self, f"s{k}")(p)

    def drain(self):
        for n in range(11):
            self.wcopy(n).wait_send()

        @pl.loop(0, NP)
        def _(p):
            self.c0(p).wait_send()
            self.c1(p).wait_send()
            self.c2(p).wait_send()

            @pl.when(self.end)
            def _():
                self.c3(p).wait_send()

            @pl.when(self.mid)
            def _():
                self.c4(p).wait_send()
                self.c5(p).wait_send()


PACE = 7
START = {2: -47, 3: -26, 4: -11, 5: 2, 6: 20, 7: 46}
AHEAD = {2: 8, 3: 3, 4: 1, 5: 0, 6: 0, 7: 0}


def kernel(x_h, dy_h, wq_h, wk_h, wv_h, wo_h, g, tab, dx, dwq, dwk, dwv, dwo, out,
           x, dy, w, qkvT, doT, kl, vl, oT, dqkvT, insem, *bufs):
    cm = Comm(g, out, *bufs)
    loads = [pltpu.make_async_copy(src, cm.wl.at[lo:lo + n, :], insem.at[i])
             for i, (src, lo, n) in enumerate(((wq_h, 0, 576), (wk_h, 576, 192), (wv_h, 768, 192), (wo_h, 960, 576)))]
    for cp in loads:
        cp.start()
    for p in range(4):
        for cp in cm.load(p):
            cp.start()
    acts = [pltpu.make_async_copy(x_h, x, insem.at[4]), pltpu.make_async_copy(dy_h, dy, insem.at[5])]
    for cp in acts:
        cp.start()
    cm.barrier()
    for cp in loads:
        cp.wait()
    cm.pack()
    for n in range(5):
        cm.wcopy(n).start()
    cm.convert(0, 2)
    cm.run(2, 0, 2)
    cm.convert(2, 6)
    cm.forward(0, 5)
    cm.forward(1, 6)
    cm.convert(6, 10)
    cm.run(2, 2, 3)
    cm.forward(2, 7)
    cm.forward(3, 8)
    cm.convert(10, NP)
    cm.run(3, 0, 2)
    cm.run(2, 3, 7)
    cm.forward(5, 9)
    cm.forward(6, 10)
    cm.run(3, 2, 3)
    cm.run(2, 7, 8)
    cm.run(4, 0, 1)
    for n in (4, 7, 8, 9, 10):
        cm.wcopy(n).wait_recv()
    cm.unpack(w)
    for cp in acts:
        cp.wait()

    @pl.loop(0, 8)
    def _(i):
        project(i, w, x, dy, tab, qkvT, doT, kl, vl)
        cm.slot(5 * i, 5)

    @pl.loop(0, 16)
    def _(j):
        attend(j, tab, qkvT, doT, kl, vl, oT, dqkvT)
        cm.slot(40 + 4 * j, 4)

    @pl.loop(0, 8)
    def _(i):
        rows = pl.ds(pl.multiple_of(i * 256, 256), 256)
        dx[rows, :] = tn(dqkvT[:, rows], w[0:960, :]).astype(BF)
        cm.slot(104 + 4 * i, 4)

    @pl.loop(0, 2)
    def _(h):
        rows = pl.ds(pl.multiple_of(288 * h, 288), 288)
        dwq[rows, :] = nn(dqkvT[rows, :], x[...])
        cm.slot(136 + 12 * h, 6)
        dwo[rows, :] = nn(oT[rows, :], dy[...])
        cm.slot(142 + 12 * h, 6)

    dkv = nn(dqkvT[576:960, :], x[...])
    dwk[...] = dkv[0:192]
    dwv[...] = dkv[192:384]

    @pl.loop(0, -(-(START[7] + PACE * NP - 160) // 4))
    def _(i):
        cm.slot(160 + 4 * i, 4)

    cm.drain()


def backward(x, dy, wq, wk, wv, wo, g, tab):
    hbm, vm = pl.BlockSpec(memory_space=pltpu.HBM), pl.BlockSpec(memory_space=pltpu.VMEM)

    def buf(*shape, dtype=BF):
        return pltpu.VMEM(shape, dtype)

    dma = pltpu.SemaphoreType.DMA
    return pl.pallas_call(
        kernel,
        out_shape=(buf(T, D), buf(576, D, dtype=F32), buf(192, D, dtype=F32), buf(192, D, dtype=F32), buf(576, D, dtype=F32),
                   buf(3, 192, D, dtype=F32)),
        in_specs=[hbm] * 7 + [vm], out_specs=[vm] * 6,
        scratch_shapes=[
            buf(T, D), buf(T, D), buf(1536, D), buf(960, T), buf(576, T), buf(3, 1024, 128), buf(3, 1024, 128), buf(576, T),
            buf(960, T), dma((6,)),
            buf(1536, 72), buf(8, 96, 1152), buf(4, 96, 1536, dtype=F32), buf(NP, 2, 4, 48, 384), buf(NP, 4, 48, 384),
            buf(NP, 2, 2, 48, 384), buf(NP, 2, 48, 384), buf(NP, 2, 48, 384), buf(NP, 48, 384), buf(NP, 48, 384),
            buf(NP, 48, 384), buf(NP, 48, 384, dtype=F32), buf(NP, 48, 384, dtype=F32), buf(NP, 48, 384, dtype=F32),
            dma((6, NP)), dma((6, NP)), dma((11,)), dma((11,)), dma((2, NP))],
        compiler_params=pltpu.CompilerParams(vmem_limit_bytes=50 * 2**20, collective_id=0, has_side_effects=True),
        name="attn_backward_and_sum",
    )(x, dy, wq, wk, wv, wo, g, tab)


def write_kernel(*refs):
    n = len(refs) // 2
    sem = refs[-1]
    copies = [pltpu.make_async_copy(refs[i], refs[n + i], sem.at[i]) for i in range(n)]
    for cp in copies:
        cp.start()
    for cp in copies:
        cp.wait()


def write_out(arrays):
    return pl.pallas_call(
        write_kernel, out_shape=[jax.ShapeDtypeStruct(a.shape, a.dtype) for a in arrays],
        in_specs=[pl.BlockSpec(memory_space=pltpu.VMEM)] * len(arrays),
        out_specs=[pl.BlockSpec(memory_space=pltpu.HBM)] * len(arrays),
        scratch_shapes=[pltpu.SemaphoreType.DMA((len(arrays),))],
        compiler_params=pltpu.CompilerParams(vmem_limit_bytes=2**20), name="write_out")(*arrays)


def solution(mesh):
    fsdp = ("row", "col")
    every = ("dp", "row", "col")

    def step(x_loc, dy_loc, wq, wk, wv, wo, g):
        def rows_first(a):
            return jnp.transpose(a, (1, 2, 0)).reshape(-1, 72)

        dx, dwq, dwk, dwv, dwo, dw_next = write_out(backward(
            x_loc.reshape(T, D), dy_loc.reshape(T, D), rows_first(wq), rows_first(wk), rows_first(wv), wo.reshape(576, 72),
            g[0], jnp.asarray(rope_tables())))

        def head_first(a, n):
            return jnp.transpose(a.reshape(n, 64, D), (2, 0, 1))[None]

        return (dx.reshape(32, 64, D), jnp.transpose(dw_next, (0, 2, 1)), head_first(dwq, 9), head_first(dwk, 3),
                head_first(dwv, 3), dwo.reshape(1, 9, 64, D))

    return jax.shard_map(
        step, mesh=mesh,
        in_specs=(P(every), P(every), P(fsdp), P(fsdp), P(fsdp), P(None, None, fsdp), P(every)),
        out_specs=(P(every), P(None, None, fsdp), P(every), P(every), P(every), P(every)),
        check_vma=False)
```

```python
import functools
import jax, jax.numpy as jnp, numpy as np
from jax import lax
from jax.experimental import pallas as pl
from jax.experimental.pallas import tpu as pltpu
from jax.sharding import PartitionSpec as P

T = 2048
D = 576
HD = 64
F32 = jnp.float32
BF = jnp.bfloat16
LOG2E = 1.4426950408889634
PR = 48
PC = 384
SCORE = (64, 384)
QKV = 960
ROWS = 1536


def rope_tables():
    pos = np.arange(64, dtype=np.float32)
    inv = np.float32(10000.0) ** (-np.arange(32, dtype=np.float32) * np.float32(2.0 / 64))
    ang = inv[:, None] * pos[None, :]
    cos, sin = np.cos(ang).astype(np.float32), np.sin(ang).astype(np.float32)
    return np.stack([np.tile(cos, (1, 4)), np.tile(sin, (1, 4))])


def nt(a, b):
    return lax.dot_general(a, b, (((1,), (1,)), ((), ())), preferred_element_type=F32)


def nn(a, b):
    return lax.dot_general(a, b, (((1,), (0,)), ((), ())), preferred_element_type=F32)


def tn(a, b):
    return lax.dot_general(a, b, (((0,), (0,)), ((), ())), preferred_element_type=F32)


def project(i, w, x, dy, tab, qkvT, doT, kl, vl):
    rows = pl.ds(pl.multiple_of(i * 256, 256), 256)
    cos, sin = tab[0], tab[1]
    raw = nt(w[0:QKV, :], x[rows, :])
    for h in range(12):
        a, b = raw[64 * h:64 * h + 32], raw[64 * h + 32:64 * h + 64]
        qkvT[64 * h:64 * h + 32, rows] = (a * cos - b * sin).astype(BF)
        qkvT[64 * h + 32:64 * h + 64, rows] = (b * cos + a * sin).astype(BF)
    qkvT[768:QKV, rows] = raw[768:QKV].astype(BF)
    doT[:, rows] = nt(w[QKV:ROWS, :], dy[rows, :]).astype(BF)
    for g in range(3):
        for src, dst in ((576, kl), (768, vl)):
            tr = qkvT[src + 64 * g:src + 64 * g + 64, rows].T
            for s in range(2):
                keys = pl.ds(pl.multiple_of(i * 128 + 64 * s, 64), 64)
                dst[g, keys, :] = jnp.concatenate([tr[128 * s:128 * s + 64], tr[128 * s + 64:128 * s + 128]], axis=1)


def attend(js, tab, qkvT, doT, kl, vl, oT, dqkvT):
    cos, sin = tab[0, :, 0:128], tab[1, :, 0:128]
    key_i = lax.broadcasted_iota(jnp.int32, SCORE, 0)
    lane = lax.broadcasted_iota(jnp.int32, SCORE, 1)
    causal = key_i <= lane % 64
    first = lane % 128 < 64
    zero = jnp.zeros(SCORE, BF)

    def blocks(v):
        return jnp.concatenate([jnp.where(first, v, zero), jnp.where(first, zero, v)], axis=0)

    loaded = []
    units = [(j, g) for j in js for g in range(3)]
    for j, g in units:
        cols = pl.ds(pl.multiple_of(j * 128, 128), 128)
        keys = pl.ds(pl.multiple_of(j * 64, 64), 64)
        heads = [64 * (3 * g + r) for r in range(3)]
        q3 = jnp.concatenate([qkvT[h:h + 64, cols] for h in heads], axis=1)
        do3 = jnp.concatenate([doT[h:h + 64, cols] for h in heads], axis=1)
        loaded.append((heads, q3, do3, nn(kl[g, keys, :], blocks(q3)), nn(vl[g, keys, :], blocks(do3))))
    soft = []
    for n in range(len(units)):
        heads, q3, do3, s, dp = loaded[n]
        s = jnp.where(causal, s * (0.125 * LOG2E), -1e30)
        e = jnp.exp2(s - jnp.max(s, axis=0, keepdims=True))
        p = e * (1.0 / jnp.sum(e, axis=0, keepdims=True))
        delta = jnp.sum(p * dp, axis=0, keepdims=True)
        ds = (p * (dp - delta) * 0.125).astype(BF)
        soft.append((blocks(p.astype(BF)), blocks(ds)))
    for n, (j, g) in enumerate(units):
        cols = pl.ds(pl.multiple_of(j * 128, 128), 128)
        heads, q3, do3, s, dp = loaded[n]
        kT = qkvT[576 + 64 * g:640 + 64 * g, cols]
        vT = qkvT[768 + 64 * g:832 + 64 * g, cols]
        pbd, dsbd = soft[n]
        o = nn(vT, pbd).astype(BF)
        dq = nn(kT, dsbd)
        for r in range(3):
            h, c = heads[r], slice(128 * r, 128 * r + 128)
            oT[h:h + 64, cols] = o[:, c]
            a, b = dq[0:32, c], dq[32:64, c]
            dqkvT[h:h + 32, cols] = (a * cos + b * sin).astype(BF)
            dqkvT[h + 32:h + 64, cols] = (b * cos - a * sin).astype(BF)
        dqkvT[768 + 64 * g:832 + 64 * g, cols] = nt(do3, pbd).astype(BF)
        dk = nt(q3, dsbd)
        a, b = dk[0:32], dk[32:64]
        dqkvT[576 + 64 * g:608 + 64 * g, cols] = (a * cos + b * sin).astype(BF)
        dqkvT[608 + 64 * g:640 + 64 * g, cols] = (b * cos - a * sin).astype(BF)


NP = 18
MESH = pl.DeviceIdType.MESH


def flip(bit, other):
    return 1 - other if bit else other


class Comm:
    def __init__(self, g, out, wl, pk, gf, gsh, d2d, u, r1, v, r2, gs, ze, za, zr, zf, ssem, rsem, wss, wsr, gsem):
        self.__dict__.update({k: val for k, val in locals().items() if k != "self"})
        self.z, self.y, self.col = lax.axis_index("dp"), lax.axis_index("row"), lax.axis_index("col")
        self.c, self.x = lax.rem(self.col, 2), lax.div(self.col, 2)
        self.sib = self.col + 1 - 2 * self.c
        self.xcol = (1 - self.x) * 2 + self.c
        self.yrow = 1 - self.y
        self.zp = self.z + 1 - 2 * lax.rem(self.z, 2)
        self.zm = 3 - self.z
        self.mid = (self.z == 1) | (self.z == 2)
        self.end = (self.z == 0) | (self.z == 3)
        self.sibling, self.xdev = (self.z, self.y, self.sib), (self.z, self.y, self.xcol)
        self.ydev, self.zdev, self.mdev = (self.z, self.yrow, self.col), (self.zp, self.y, self.col), (self.zm, self.y, self.col)

    def barrier(self):
        sem = pltpu.get_barrier_semaphore()
        for dev in (self.sibling, self.xdev, self.ydev, self.zdev):
            pl.semaphore_signal(sem, inc=1, device_id=dev, device_id_type=MESH)

        @pl.when(self.mid)
        def _():
            pl.semaphore_signal(sem, inc=1, device_id=self.mdev, device_id_type=MESH)

        pl.semaphore_wait(sem, 4 + lax.rem(lax.div(self.z + 1, 2), 2))

    def pack(self):
        mine = 4 * self.y + self.col
        self.pk[mine] = jnp.concatenate([self.wl[96 * j:96 * j + 96, :] for j in range(16)], axis=1)

    def unpack(self, w):
        for j in range(16):
            w[96 * j:96 * j + 96, :] = jnp.concatenate([self.pk[i, :, 72 * j:72 * j + 72] for i in range(8)], axis=1)

    def wcopy(self, n):
        me = 4 * self.y + self.col
        fx, fy, fd = 4 * self.y + self.xcol, 4 * self.yrow + self.col, 4 * self.yrow + self.xcol
        slab, lo, size, dev = (
            (me, 0, 48, self.xdev), (me, 48, 48, self.ydev), (me, 48, 48, self.xdev), (me, 0, 48, self.ydev),
            (me, 0, 96, self.sibling),
            (fx, 0, 48, self.ydev), (fy, 48, 48, self.xdev),
            (fx, 0, 96, self.sibling), (fy, 0, 96, self.sibling),
            (fd, 0, 48, self.sibling), (fd, 48, 48, self.sibling))[n]
        ref = self.pk.at[slab, pl.ds(lo, size), :]
        return pltpu.make_async_remote_copy(ref, ref, self.wss.at[n], self.wsr.at[n], device_id=dev, device_id_type=MESH)

    def load(self, p):
        k, r, slot = lax.div(p, 6), lax.rem(p, 6), lax.rem(p, 4)
        return [pltpu.make_async_copy(self.g.at[k, pl.ds(pl.multiple_of(288 * h + 48 * r, 48), 48), :],
                                      self.gf.at[slot, pl.ds(48 * h, 48), :], self.gsem.at[h, p]) for h in range(2)]

    def remote(self, n, src, dst, p, dev):
        return pltpu.make_async_remote_copy(src, dst, self.ssem.at[n, p], self.rsem.at[n, p], device_id=dev, device_id_type=MESH)

    def c0(self, p):
        return self.remote(0, self.gsh.at[p, 1], self.d2d.at[p], p, self.sibling)

    def c1(self, p):
        t = lax.rem(p, 2)
        dev = (self.z, self.y + t * (self.yrow - self.y), self.xcol + t * (self.col - self.xcol))
        return self.remote(1, self.u.at[p, 1], self.r1.at[p], p, dev)

    def c2(self, p):
        t = lax.rem(p, 2)
        dev = (self.z, self.yrow + t * (self.y - self.yrow), self.col + t * (self.xcol - self.col))
        return self.remote(2, self.v.at[p, 1], self.r2.at[p], p, dev)

    def c3(self, p):
        return self.remote(3, self.gs.at[p], self.ze.at[p], p, self.zdev)

    def c4(self, p):
        return self.remote(4, self.za.at[p], self.zr.at[p], p, self.mdev)

    def c5(self, p):
        return self.remote(5, self.zf.at[p], self.zr.at[p], p, self.zdev)

    def s1(self, p):
        for cp in self.load(p):
            cp.wait()
        slot = lax.rem(p, 4)
        for q in range(4):
            top = self.gf[slot, 0:PR, PC * q:384 * q + 384].astype(BF)
            bot = self.gf[slot, 48:96, 384 * q:384 * q + 384].astype(BF)
            for cc in range(2):
                lanes = slice(192 * cc, 192 * cc + 192)
                self.gsh[p, flip(cc, self.c), q] = jnp.concatenate([top[:, lanes], bot[:, lanes]], axis=1)
        self.c0(p).start()

        @pl.when(p + 4 < NP)
        def _():
            for cp in self.load(p + 4):
                cp.start()

    def convert(self, lo, hi):
        @pl.loop(lo, hi)
        def _(p):
            self.s1(p)

    def forward(self, got, send):
        self.wcopy(got).wait_recv()
        self.wcopy(send).start()

    def s2(self, p):
        self.c0(p).wait_recv()
        t = lax.rem(p, 2)
        for yy in range(2):
            for xx in range(2):
                q = 2 * yy + xx
                fx, fy = flip(xx, self.x), flip(yy, self.y)
                self.u[p, fx + t * (fy - fx), yy + t * (xx - yy)] = self.gsh[p, 0, q] + self.d2d[p, q]
        self.c1(p).start()

    def s3(self, p):
        self.c1(p).wait_recv()
        t = lax.rem(p, 2)
        own = self.y + t * (self.x - self.y)
        for e in range(2):
            self.v[p, flip(e, own)] = self.u[p, 0, e] + self.r1[p, e]
        self.c2(p).start()

    def s4(self, p):
        self.c2(p).wait_recv()
        self.gs[p] = self.v[p, 0] + self.r2[p]

        @pl.when(self.end)
        def _():
            self.c3(p).start()

    def s5(self, p):
        @pl.when(self.mid)
        def _():
            self.c3(p).wait_recv()
            self.za[p] = self.gs[p].astype(F32) + self.ze[p].astype(F32)
            self.c4(p).start()

    def s6(self, p):
        @pl.when(self.mid)
        def _():
            self.c4(p).wait_recv()
            self.zf[p] = self.za[p] + self.zr[p]
            self.c5(p).start()

            @pl.when(lax.rem(p, 6) == 5)
            def _():
                self.emit(self.zf, lax.div(p, 6))

    def s7(self, p):
        @pl.when(self.end)
        def _():
            self.c5(p).wait_recv()

            @pl.when(lax.rem(p, 6) == 5)
            def _():
                self.emit(self.zr, lax.div(p, 6))

    def emit(self, buf, k):
        tr = buf[pl.ds(6 * k, 6)].reshape(288, 384).T
        self.out[k] = jnp.concatenate([tr[0:192], tr[192:384]], axis=1)

    def slot(self, now, length):
        for k in (7, 6, 5, 4, 3, 2):
            first = now - START[k] + 20 * PACE[k]
            lo = lax.max(lax.div(first, PACE[k]) - 20, AHEAD[k])
            self.run(k, lo, lax.min(lax.div(first + length, PACE[k]) - 20, NP))

    def run(self, k, lo, hi):
        @pl.loop(lo, hi)
        def _(p):
            getattr(self, f"s{k}")(p)

    def drain(self):
        for n in range(11):
            self.wcopy(n).wait_send()

        @pl.loop(0, NP)
        def _(p):
            self.c0(p).wait_send()
            self.c1(p).wait_send()
            self.c2(p).wait_send()

            @pl.when(self.end)
            def _():
                self.c3(p).wait_send()

            @pl.when(self.mid)
            def _():
                self.c4(p).wait_send()
                self.c5(p).wait_send()


START = {2: -56, 3: -28, 4: -14, 5: -2, 6: 16, 7: 42}
PACE = {2: 7, 3: 7, 4: 7, 5: 7, 6: 7, 7: 7}
AHEAD = {2: 8, 3: 4, 4: 2, 5: 0, 6: 0, 7: 0}
SLICE = {"project": 5, "attend": 4, "dx": 7, "dw": 6, "tail": 4}


def kernel(x_h, dy_h, wq_h, wk_h, wv_h, wo_h, g, tab_h, dx, dwq, dwk, dwv, dwo, out,
           x, dy, w, qkvT, doT, kl, vl, oT, dqkvT, tab, insem, *bufs):
    cm = Comm(g, out, *bufs)
    loads = [pltpu.make_async_copy(src, cm.wl.at[lo:lo + n, :], insem.at[i])
             for i, (src, lo, n) in enumerate(((wq_h, 0, 576), (wk_h, 576, 192), (wv_h, 768, 192), (wo_h, QKV, 576)))]
    for cp in loads:
        cp.start()
    for p in range(4):
        for cp in cm.load(p):
            cp.start()
    acts = [pltpu.make_async_copy(x_h, x, insem.at[4]), pltpu.make_async_copy(dy_h, dy, insem.at[5]),
            pltpu.make_async_copy(tab_h, tab, insem.at[6])]
    for cp in acts:
        cp.start()
    cm.barrier()
    for cp in loads:
        cp.wait()
    cm.pack()
    cm.wcopy(0).start()
    cm.wcopy(1).start()
    cm.wcopy(4).start()
    cm.convert(0, 2)
    cm.run(2, 0, 2)
    cm.wcopy(2).start()
    cm.wcopy(3).start()
    cm.convert(2, 4)
    cm.forward(0, 5)
    cm.forward(1, 6)
    cm.convert(4, 8)
    cm.run(2, 2, 4)
    cm.forward(2, 7)
    cm.forward(3, 8)
    cm.convert(8, 12)
    cm.run(3, 0, 2)
    cm.convert(12, 18)
    cm.run(2, 4, 6)
    cm.forward(5, 9)
    cm.forward(6, 10)
    cm.run(4, 0, 2)
    cm.run(3, 2, 4)
    cm.run(2, 6, 8)
    for n in (4, 7, 8, 9, 10):
        cm.wcopy(n).wait_recv()
    cm.unpack(w)
    for cp in acts:
        cp.wait()

    long = SLICE["project"]

    @pl.loop(0, 8)
    def _(i):
        project(i, w, x, dy, tab, qkvT, doT, kl, vl)
        cm.slot(long * i, long)

    at1 = 8 * long
    long1 = SLICE["attend"]

    @pl.loop(0, 16)
    def _(j):
        attend((j,), tab, qkvT, doT, kl, vl, oT, dqkvT)
        cm.slot(at1 + long1 * j, long1)

    at2 = at1 + 16 * long1
    long2 = SLICE["dx"]

    @pl.loop(0, 4)
    def _(i):
        rows = pl.ds(pl.multiple_of(i * 512, 512), 512)
        dx[rows, :] = tn(dqkvT[:, rows], w[0:QKV, :]).astype(BF)
        cm.slot(at2 + long2 * i, long2)

    at3 = at2 + 4 * long2
    long3 = SLICE["dw"]

    @pl.loop(0, 2)
    def _(h):
        rows = pl.ds(pl.multiple_of(288 * h, 288), 288)
        dwq[rows, :] = nn(dqkvT[rows, :], x[...])
        cm.slot(at3 + 2 * long3 * h, long3)
        dwo[rows, :] = nn(oT[rows, :], dy[...])
        cm.slot(at3 + 2 * long3 * h + long3, long3)

    dkv = nn(dqkvT[576:QKV, :], x[...])
    dwk[...] = dkv[0:192]
    dwv[...] = dkv[192:384]
    at4 = at3 + 4 * long3
    long4 = SLICE["tail"]

    @pl.loop(0, -(-(START[7] + PACE[7] * NP - at4) // long4))
    def _(i):
        cm.slot(at4 + long4 * i, long4)

    cm.drain()


def backward(x, dy, wq, wk, wv, wo, g, tab):
    hbm, vm = pl.BlockSpec(memory_space=pltpu.HBM), pl.BlockSpec(memory_space=pltpu.VMEM)

    def buf(*shape, dtype=BF):
        return pltpu.VMEM(shape, dtype)

    dma = pltpu.SemaphoreType.DMA
    return pl.pallas_call(
        kernel,
        out_shape=(buf(T, D), buf(576, D, dtype=F32), buf(192, D, dtype=F32), buf(192, D, dtype=F32), buf(576, D, dtype=F32),
                   buf(3, 192, D, dtype=F32)),
        in_specs=[hbm] * 8, out_specs=[vm] * 6,
        scratch_shapes=[
            buf(T, D), buf(T, D), buf(ROWS, D), buf(QKV, T), buf(576, T), buf(3, 1024, 128), buf(3, 1024, 128), buf(576, T),
            buf(QKV, T), buf(2, 32, 256, dtype=F32), dma((7,)),
            buf(ROWS, 72), buf(8, 96, 1152), buf(4, 96, ROWS, dtype=F32), buf(NP, 2, 4, PR, PC), buf(NP, 4, PR, PC),
            buf(NP, 2, 2, PR, PC), buf(NP, 2, PR, PC), buf(NP, 2, PR, PC), buf(NP, PR, PC), buf(NP, PR, PC),
            buf(NP, PR, PC), buf(NP, PR, PC, dtype=F32), buf(NP, PR, PC, dtype=F32), buf(NP, PR, PC, dtype=F32),
            dma((6, NP)), dma((6, NP)), dma((11,)), dma((11,)), dma((2, NP))],
        compiler_params=pltpu.CompilerParams(vmem_limit_bytes=50 * 2**20, collective_id=0, has_side_effects=True),
        name="attn_backward_and_sum",
    )(x, dy, wq, wk, wv, wo, g, tab)


def write_kernel(*refs):
    n = len(refs) // 2
    sem = refs[-1]
    copies = [pltpu.make_async_copy(refs[i], refs[n + i], sem.at[i]) for i in range(n)]
    for cp in copies:
        cp.start()
    for cp in copies:
        cp.wait()


def write_out(arrays):
    return pl.pallas_call(
        write_kernel, out_shape=[jax.ShapeDtypeStruct(a.shape, a.dtype) for a in arrays],
        in_specs=[pl.BlockSpec(memory_space=pltpu.VMEM)] * len(arrays),
        out_specs=[pl.BlockSpec(memory_space=pltpu.HBM)] * len(arrays),
        scratch_shapes=[pltpu.SemaphoreType.DMA((len(arrays),))],
        compiler_params=pltpu.CompilerParams(vmem_limit_bytes=2**20), name="write_out")(*arrays)


def solution(mesh):
    fsdp = ("row", "col")
    every = ("dp", "row", "col")

    def step(x_loc, dy_loc, wq, wk, wv, wo, g):
        def rows_first(a):
            return jnp.transpose(a, (1, 2, 0)).reshape(-1, 72)

        dx, dwq, dwk, dwv, dwo, dw_next = write_out(backward(
            x_loc.reshape(T, D), dy_loc.reshape(T, D), rows_first(wq), rows_first(wk), rows_first(wv), wo.reshape(576, 72),
            g[0], jnp.asarray(rope_tables())))

        def head_first(a, n):
            return jnp.transpose(a.reshape(n, 64, D), (2, 0, 1))[None]

        return (dx.reshape(32, 64, D), jnp.transpose(dw_next, (0, 2, 1)), head_first(dwq, 9), head_first(dwk, 3),
                head_first(dwv, 3), dwo.reshape(1, 9, 64, D))

    return jax.shard_map(
        step, mesh=mesh,
        in_specs=(P(every), P(every), P(fsdp), P(fsdp), P(fsdp), P(None, None, fsdp), P(every)),
        out_specs=(P(every), P(None, None, fsdp), P(every), P(every), P(every), P(every)),
        check_vma=False)
```
